32 devices in a mesh: group: 2 (over y), expert: 4 (over x, core), tensor: 4 (over z).
Axes of the slice: x: 2, y: 2, z: 4, core: 2. Of those that a mesh axis runs over, the one named last changes fastest.
Arguments:
- tokens: bfloat16 [512, 4096], P(('group', 'expert'), 'tensor'), parts along dimension 0, may hold values from -6 to 6
- w_gate: bfloat16 [8, 4096, 1536], P('expert', 'tensor'), may hold values from -0.125 to 0.125
- w_up: bfloat16 [8, 4096, 1536], P('expert', 'tensor'), may hold values from -0.125 to 0.125
- w_down: bfloat16 [8, 1536, 4096], P('expert', None, 'tensor'), may hold values from -0.15625 to 0.15625
- expert_ids: int32 [512, 8], P(('group', 'expert')), parts along dimension 0, may hold values from 0 to 7, as said below
- route_weights: float32 [512, 8], P(('group', 'expert')), parts along dimension 0, may hold values from 0.05 to 0.5
Outputs:
- mixed_out: bfloat16 [512, 4096], P(('group', 'expert'), 'tensor'), parts along dimension 0
The draws below stay inside these ranges and needn't reach their ends.
There are 2 independent parts, one for each index of `group`. The reference program is written for one: setup_inputs(seed, part) draws one part's arguments, and reference() takes and returns one part's arrays. A program takes and returns all parts, laid end to end along the dimension named above; an argument that names none is the same for every part. Nothing has to cross between parts.
Inputs may be any that keep to these rules, and one draw needn't show every extreme that they name: `expert_ids`: each row names 8 different experts. In each aligned block of 64 rows no expert is named by more than 64 rows, and one expert, the same in every block of a part, is named by exactly 64 rows of every block.
All inputs are finite; a program needn't handle non-finite values.
Results may differ from the reference program's by a relative error of at most 0.0057.
Values may be sent and summed in bfloat16 or wider, within the bound.
A program may use at most 128 MiB of HBM per device.

```python
import math
import jax
import jax.numpy as jnp
from jax import lax

D = 4096
FF = 1536
TOP = 8
TOK_DEV = 64
EXPERTS = 8
TOKENS = 256
BLOCKS = 4
CAP = 64


def expert_of(ordinal, hot_expert):
    return ordinal + (ordinal >= hot_expert).astype(jnp.int32)


def draw_expert_ids(key, part):
    hot_expert = jax.random.randint(jax.random.fold_in(key, 11), (), 0, EXPERTS, dtype=jnp.int32)
    pool_size = (EXPERTS - 1) * CAP
    deficit_total = EXPERTS * CAP - TOK_DEV * TOP
    block_keys = jax.random.split(jax.random.fold_in(key, 12), BLOCKS)

    def column_order(column_key):
        return jax.random.permutation(column_key, TOP).astype(jnp.int32)

    def one_block(block_key):
        sub_keys = jax.random.split(block_key, 3)
        shuffled = jax.random.permutation(sub_keys[0], pool_size).astype(jnp.int32)
        chosen = shuffled[:deficit_total] // CAP
        labels = jnp.arange(EXPERTS - 1, dtype=jnp.int32)
        deficit = jnp.sum((chosen[:, None] == labels[None, :]).astype(jnp.int32), axis=0)
        others = CAP - deficit
        counts = jnp.zeros((EXPERTS,), jnp.int32).at[expert_of(labels, hot_expert)].set(others)
        counts = counts.at[hot_expert].set(CAP)
        run_ends = jnp.cumsum(counts)
        position = jnp.arange(TOK_DEV * TOP, dtype=jnp.int32)
        sequence = jnp.sum((run_ends[None, :] <= position[:, None]).astype(jnp.int32), axis=1)
        layout = sequence.reshape(TOP, TOK_DEV).T
        row_order = jax.random.permutation(sub_keys[1], TOK_DEV).astype(jnp.int32)
        layout = layout[row_order]
        columns = jax.vmap(column_order)(jax.random.split(sub_keys[2], TOK_DEV))
        return jnp.take_along_axis(layout, columns, axis=1)
    return jax.vmap(one_block)(block_keys).reshape(TOKENS, TOP).astype(jnp.int32)


def with_spikes(entries, stream_key, source, target, shards_of, factor):
    owner, partner = [(jnp.arange(entries.shape[dim]) // (entries.shape[dim] // shards_of)).reshape([-1 if axis == dim else 1 for axis in range(entries.ndim)]) for dim in (source, target)]
    chosen = jax.random.permutation(stream_key, shards_of)[partner]
    strong = (owner == chosen) | (owner == (partner + shards_of // 2) % shards_of)
    return jnp.where(strong, factor * entries, entries)


def levels(own_key, shape, cuts, least, top_value):
    loudness, own = 1.0, jax.random.fold_in(own_key, 6)
    for dim, blocks in cuts:
        heights = jnp.exp(jax.random.uniform(jax.random.fold_in(own, dim), (blocks,), jnp.float32, least / len(cuts), top_value / len(cuts)))
        loudness = loudness * jnp.repeat(heights, shape[dim] // blocks).reshape([-1 if axis == dim else 1 for axis in range(len(shape))])
    return loudness


def scatter_about(rng, dims, width, bound, cuts=(), held_as=jnp.bfloat16):
    result = jax.random.normal(rng, dims, jnp.float32) * width
    if len(cuts) > 0:
        result = levels(rng, dims, cuts, -0.22, 0.18) * result
    return jnp.clip(result, min=-bound, max=bound).astype(held_as)


def bell_draw_with(rng, extent, deviation, bound, pieces, heavy, kind=jnp.bfloat16):
    values = deviation * jax.random.normal(rng, extent, jnp.float32)
    if pieces:
        values = values * levels(rng, extent, pieces, -0.22, 0.18)
    return jnp.clip(with_spikes(values, jax.random.fold_in(rng, 3), *heavy), -bound, bound).astype(kind)


def setup_inputs(seed: int = 0, part: int = 0) -> dict:
    keys = jax.random.split(jax.random.key(seed), 7)
    part_splits = jax.random.split(jax.random.fold_in(keys[6], part), 7)
    tokens = scatter_about(part_splits[0], (TOKENS, D), 1.0, 6.0, ((0, 4), (1, 4)))
    w_gate = bell_draw_with(keys[1], (EXPERTS, D, FF), D ** -0.5, 0.125, ((0, 4), (1, 4)), (1, 2, 4, 2.0))
    w_up = bell_draw_with(keys[2], (EXPERTS, D, FF), D ** -0.5, 0.125, ((0, 4), (1, 4)), (1, 2, 4, 2.0))
    w_down = scatter_about(keys[3], (EXPERTS, FF, D), FF ** -0.5, 0.15625, ((0, 4), (2, 4)))
    expert_ids = draw_expert_ids(jax.random.fold_in(jax.random.fold_in(keys[6], part), 71), part)
    route_weights = jnp.clip(jnp.exp(math.log(0.5) - 2.3025851 * jax.random.uniform(part_splits[5], (TOKENS, TOP), jnp.float32) ** levels(part_splits[5], (TOKENS, TOP), ((0, 4),), -0.2, 0.2)), 0.05, 0.5)
    return dict(tokens=tokens, w_gate=w_gate, w_up=w_up, w_down=w_down, expert_ids=expert_ids, route_weights=route_weights)


def slot_numbers(expert_ids):
    flat_ids = expert_ids.reshape(BLOCKS, TOK_DEV * TOP)
    labels = jnp.arange(EXPERTS, dtype=jnp.int32)
    onehot = (flat_ids[:, :, None] == labels[None, None, :]).astype(jnp.int32)
    before = jnp.cumsum(onehot, axis=1) - onehot
    return jnp.sum(before * onehot, axis=2).reshape(TOKENS, TOP).astype(jnp.int32)


def expert_block(operands):
    row_block, gate_w, up_w, down_w = operands
    gate = jnp.dot(row_block, gate_w, preferred_element_type=jnp.float32)
    up = jnp.dot(row_block, up_w, preferred_element_type=jnp.float32)
    hidden = (jax.nn.silu(gate) * up).astype(jnp.bfloat16)
    return jnp.dot(hidden, down_w, preferred_element_type=jnp.float32).astype(jnp.bfloat16)


def reference(tokens, w_gate, w_up, w_down, expert_ids, route_weights):
    slot_ids = slot_numbers(expert_ids)
    block_ids = (jnp.arange(TOKENS, dtype=jnp.int32) // TOK_DEV)[:, None] * jnp.ones((1, TOP), jnp.int32)
    position = ((expert_ids * BLOCKS + block_ids) * CAP + slot_ids).reshape(TOKENS * TOP).astype(jnp.int32)
    owners = (jnp.arange(TOKENS, dtype=jnp.int32)[:, None] * jnp.ones((1, TOP), jnp.int32)).reshape(TOKENS * TOP)
    source = jnp.full((EXPERTS * BLOCKS * CAP,), -1, jnp.int32).at[position].set(owners)
    gathered = tokens[jnp.maximum(source, 0)]
    expert_input = jnp.where((source >= 0)[:, None], gathered, jnp.zeros((), jnp.bfloat16))
    expert_input = expert_input.reshape(EXPERTS, BLOCKS * CAP, D)
    expert_output = lax.map(expert_block, (expert_input, w_gate, w_up, w_down))
    expert_output = expert_output.reshape(EXPERTS * BLOCKS * CAP, D)
    picked = expert_output[position].reshape(TOKENS, TOP, D).astype(jnp.float32)
    mixed_out = jnp.sum(picked * route_weights[:, :, None], axis=1)
    return mixed_out.astype(jnp.bfloat16)
```

```python
import functools

import jax
import jax.numpy as jnp
from jax import lax
from jax.experimental import pallas as pl
from jax.experimental.pallas import tpu as pltpu
from jax.sharding import PartitionSpec as P


def slot_numbers(flat_ids, experts_all):
    labels = jnp.arange(experts_all, dtype=jnp.int32)
    onehot = (flat_ids[:, None] == labels[None, :]).astype(jnp.int32)
    before = jnp.cumsum(onehot, axis=0) - onehot
    return jnp.sum(before * onehot, axis=1)


def routed_by_slots(tokens, w_gate, w_up, w_down, expert_ids, route_weights):
    n_expert = lax.axis_size("expert")
    held_experts = w_gate.shape[0]
    experts_all = held_experts * n_expert
    tok_rows = tokens.shape[0]
    col_share = tokens.shape[1]
    per_token = expert_ids.shape[1]
    capacity = min(tok_rows, 2 * tok_rows * per_token // experts_all)
    flat_ids = expert_ids.reshape(tok_rows * per_token)
    position = flat_ids * capacity + slot_numbers(flat_ids, experts_all)
    owners = jnp.arange(tok_rows * per_token, dtype=jnp.int32) // per_token
    source = jnp.full((experts_all * capacity,), -1, jnp.int32).at[position].set(owners)
    filled = (source >= 0)[:, None]
    picked_rows = jnp.where(filled, tokens[jnp.maximum(source, 0)], jnp.zeros((), tokens.dtype))
    outgoing = picked_rows.reshape(n_expert, held_experts, capacity, col_share)
    received = lax.all_to_all(outgoing, "expert", split_axis=0, concat_axis=0, tiled=True)
    gate_part = jnp.einsum("sjnd,jdf->sjnf", received, w_gate, preferred_element_type=jnp.float32)
    up_part = jnp.einsum("sjnd,jdf->sjnf", received, w_up, preferred_element_type=jnp.float32)
    gate_share = lax.psum_scatter(gate_part, "tensor", scatter_dimension=3, tiled=True)
    up_share = lax.psum_scatter(up_part, "tensor", scatter_dimension=3, tiled=True)
    hidden_share = (jax.nn.silu(gate_share) * up_share).astype(jnp.bfloat16)
    hidden = lax.all_gather(hidden_share, "tensor", axis=3, tiled=True)
    result = jnp.einsum("sjnf,jfd->sjnd", hidden, w_down, preferred_element_type=jnp.float32)
    returned = result.astype(jnp.bfloat16)
    combined = lax.all_to_all(returned, "expert", split_axis=0, concat_axis=0, tiled=True).reshape(
        experts_all * capacity, col_share
    )
    picked = combined[position].reshape(tok_rows, per_token, col_share).astype(jnp.float32)
    mixed_out = jnp.sum(picked * route_weights[:, :, None], axis=1)
    return mixed_out.astype(jnp.bfloat16)


LANES = 128
CHUNK = 256
RS_LAG = 2
AG_LAG = 2
HEAD_OWN = 3
HEAD_PARTNER = 2
OUT_WIDTH = 512
MESH = pl.DeviceIdType.MESH


def layer_kernel(
    n_expert, n_tensor, tok_hbm, ids_hbm, weights_hbm, wg_hbm, wu_hbm, wd_hbm, out_ref,
    rows_ref, ids_ref, weights_ref, route_ref, routes_ref, scale_ref, wg_ref, wu_ref, wd_ref, part_ref, sent_ref,
    got_ref, hidden_ref, acc_ref, pair_ref, far_out_ref, far_in_ref,
    in_sem, w_sem, wd_sem, tok_send, tok_recv, pass_send, route_send, route_recv, rs_send, rs_recv, ag_send, ag_recv,
    pair_send, pair_recv, home_send, home_recv,
):
    held, depth, ff = wg_hbm.shape
    tok_rows, cols = tok_hbm.shape
    all_rows = n_expert * tok_rows
    per_expert = ff // CHUNK
    half = held * per_expert // 2
    items = n_expert * half
    me = lax.axis_index("expert")
    at = lax.axis_index("tensor")
    last = n_tensor - 1
    peers = [lax.rem(me + k, n_expert) for k in range(1, n_expert)]
    chips = n_expert // 2
    core = lax.rem(me, 2)
    chip = me // 2
    partner = 2 * chip + 1 - core
    same = [2 * lax.rem(chip + k, chips) + core for k in range(chips)]
    other = [2 * lax.rem(chip + k, chips) + 1 - core for k in range(chips)]

    segments = [(me, 0, HEAD_OWN), (partner, 0, HEAD_PARTNER)]
    for k in range(1, chips):
        segments += [(same[k], 0, half), (other[k], 0, half)]
    segments += [(partner, HEAD_PARTNER, half - HEAD_PARTNER), (me, HEAD_OWN, half - HEAD_OWN)]
    starts = [sum(count for _, _, count in segments[:n]) for n in range(len(segments))]
    ends = [start + segment[2] - 1 for start, segment in zip(starts, segments)]

    def item(i):
        block, chunk = me, i
        for start, (owner, first, _) in list(zip(starts, segments))[1:]:
            past = i >= start
            block = jnp.where(past, owner, block)
            chunk = jnp.where(past, i - start + first, chunk)
        return block, chunk

    def place(f, c):
        q = f * half + c
        return q // per_expert, pl.multiple_of(lax.rem(q, per_expert) * CHUNK, CHUNK)

    def w_copy(k, f, c):
        j, start = place(f, c)
        src = (wg_hbm, wu_hbm)[k].at[j, :, pl.ds(start, CHUNK)]
        return pltpu.make_async_copy(src, (wg_ref, wu_ref)[k].at[f, c], w_sem.at[k, f, c])

    def wd_copy(f, c):
        j, start = place(f, c)
        return pltpu.make_async_copy(wd_hbm.at[j, pl.ds(start, CHUNK), :], wd_ref.at[f, c], wd_sem.at[f, c])

    own_copies = [
        pltpu.make_async_copy(tok_hbm, rows_ref.at[me], in_sem.at[0]),
        pltpu.make_async_copy(ids_hbm, ids_ref, in_sem.at[1]),
        pltpu.make_async_copy(weights_hbm, weights_ref, in_sem.at[2]),
    ]
    for copy in own_copies:
        copy.start()
    for f in range(2):
        for k in range(2):
            w_copy(k, f, 0).start()

    barrier = pltpu.get_barrier_semaphore()
    for peer in peers:
        pl.semaphore_signal(barrier, inc=1, device_id={"expert": peer}, device_id_type=MESH)

    @pl.when(at > 0)
    def _():
        pl.semaphore_signal(barrier, inc=1, device_id={"tensor": at - 1}, device_id_type=MESH)

    @pl.when(at < last)
    def _():
        pl.semaphore_signal(barrier, inc=1, device_id={"tensor": at + 1}, device_id_type=MESH)

    for copy in own_copies:
        copy.wait()
    labels = lax.broadcasted_iota(jnp.int32, route_ref.shape, 0)
    routes = jnp.zeros(route_ref.shape, jnp.float32)
    for k in range(ids_ref.shape[0]):
        routes += jnp.where(ids_ref[k:k + 1, :] == labels, weights_ref[k:k + 1, :], 0.0)
    route_ref[...] = routes
    routes_ref[me] = routes

    greeted = (n_expert - 1) + (at > 0).astype(jnp.int32) + (at < last).astype(jnp.int32)
    pl.semaphore_wait(barrier, greeted)

    def tok_copy(k, slot):
        return pltpu.make_async_remote_copy(
            src_ref=rows_ref.at[slot], dst_ref=rows_ref.at[slot], send_sem=tok_send.at[k], recv_sem=tok_recv.at[slot],
            device_id={"expert": same[k] if k else partner}, device_id_type=MESH)

    def pass_copy(k, slot):
        return pltpu.make_async_remote_copy(
            src_ref=rows_ref.at[slot], dst_ref=rows_ref.at[slot], send_sem=pass_send.at[k],
            recv_sem=tok_recv.at[slot], device_id={"expert": partner}, device_id_type=MESH)

    def route_copy(k, slot):
        return pltpu.make_async_remote_copy(
            src_ref=route_ref, dst_ref=routes_ref.at[slot], send_sem=route_send.at[k], recv_sem=route_recv.at[slot],
            device_id={"expert": peers[k]}, device_id_type=MESH)

    for k in range(chips - 1, -1, -1):
        tok_copy(k, me).start()
    for k in range(n_expert - 1):
        route_copy(k, me).start()

    def load_rest(c, carry):
        for f in range(2):
            for k in range(2):
                w_copy(k, f, c).start()
        return carry

    lax.fori_loop(1, half, load_rest, 0)

    def load_down(c, carry):
        for f in range(2):
            wd_copy(f, c).start()
        return carry

    lax.fori_loop(0, half, load_down, 0)
    acc_ref[...] = jnp.zeros_like(acc_ref)

    def far_of(f):
        return jnp.where(f == 0, last - at, at)

    def onward(f):
        return jnp.where(f == 0, jnp.maximum(at - 1, 0), jnp.minimum(at + 1, last))

    def back(f):
        return jnp.where(f == 0, jnp.minimum(at + 1, last), jnp.maximum(at - 1, 0))

    near = jnp.where(at + at < n_tensor, 1, 0)
    order = (near, 1 - near)
    nearest = jnp.minimum(at, last - at)

    def rs_copy(f, i):
        return pltpu.make_async_remote_copy(
            src_ref=sent_ref.at[f, i], dst_ref=got_ref.at[f, i], send_sem=rs_send.at[f, i], recv_sem=rs_recv.at[f, i],
            device_id={"tensor": onward(f)}, device_id_type=MESH)

    def ag_copy(f, i):
        return pltpu.make_async_remote_copy(
            src_ref=hidden_ref.at[f, i], dst_ref=hidden_ref.at[f, i], send_sem=ag_send.at[f, i],
            recv_sem=ag_recv.at[f, i], device_id={"tensor": back(f)}, device_id_type=MESH)

    def wait_weights(c):
        for f in range(2):
            for k in range(2):
                w_copy(k, f, c).wait()

    def part_of_block(block, c):
        for f in range(2):
            for k, w_ref in enumerate((wg_ref, wu_ref)):
                part_ref[f, c, block, :, k * CHUNK:(k + 1) * CHUNK] = jnp.dot(
                    rows_ref[block], w_ref[f, c], preferred_element_type=jnp.float32)

    def part_of_all(c):
        for f in range(2):
            for k, w_ref in enumerate((wg_ref, wu_ref)):
                product = jnp.dot(
                    rows_ref[...].reshape(all_rows, depth), w_ref[f, c], preferred_element_type=jnp.float32)
                part_ref[f, c, :, :, k * CHUNK:(k + 1) * CHUNK] = product.reshape(n_expert, tok_rows, CHUNK)

    def prepare(i):
        @pl.when(i < HEAD_OWN)
        def _():
            wait_weights(i)

        @pl.when(i < HEAD_OWN + HEAD_PARTNER)
        def _():
            @pl.when(i == HEAD_OWN)
            def _():
                tok_copy(0, partner).wait_recv()

            block, c = item(i)
            part_of_block(block, c)

        @pl.when(i == HEAD_OWN + HEAD_PARTNER)
        def _():
            for k in range(1, chips):
                tok_copy(k, same[k]).wait_recv()
                pass_copy(k, same[k]).start()
            for k in range(1, chips):
                pass_copy(k, other[k]).wait_recv()

        @pl.when((i >= HEAD_OWN + HEAD_PARTNER) & (i < HEAD_OWN + HEAD_PARTNER + half))
        def _():
            c = i - (HEAD_OWN + HEAD_PARTNER)

            @pl.when(c >= HEAD_OWN)
            def _():
                wait_weights(c)

            part_of_all(c)

    def reduce_item(f, i):
        far = far_of(f)
        block, c = item(i)

        @pl.when(far == 0)
        def _():
            sent_ref[f, i] = part_ref[f, c, block].astype(jnp.bfloat16)

        @pl.when(far > 0)
        def _():
            rs_copy(f, i).wait_recv()

        @pl.when((far > 0) & (far < last))
        def _():
            sent_ref[f, i] = (part_ref[f, c, block] + got_ref[f, i].astype(jnp.float32)).astype(jnp.bfloat16)

        @pl.when(far < last)
        def _():
            rs_copy(f, i).start()

        @pl.when(far == last)
        def _():
            whole = part_ref[f, c, block] + got_ref[f, i].astype(jnp.float32)
            gate = whole[:, :CHUNK]
            up = whole[:, CHUNK:]
            j, _ = place(f, c)
            weight = jnp.concatenate([scale_ref[j, block]] * (CHUNK // LANES), axis=1)
            hidden_ref[f, i] = (jax.nn.silu(gate) * up * weight).astype(jnp.bfloat16)
            ag_copy(f, i).start()

    def scales():
        for k in range(n_expert - 1):
            route_copy(k, peers[k]).wait_recv()
        row = lax.broadcasted_iota(jnp.int32, (tok_rows, tok_rows), 0)
        column = lax.broadcasted_iota(jnp.int32, (tok_rows, tok_rows), 1)
        for j in range(held):
            for b in range(n_expert):
                mine = jnp.sum(
                    jnp.where(labels == me * held + j, routes_ref[b], 0.0), axis=0, keepdims=True)
                turned = jnp.sum(
                    jnp.where(row == column, jnp.broadcast_to(mine, (tok_rows, tok_rows)), 0.0), axis=1, keepdims=True)
                scale_ref[j, b] = jnp.broadcast_to(turned, (tok_rows, LANES))

    def wait_down(c, carry):
        for f in range(2):
            wd_copy(f, c).wait()
        return carry

    def down(f, i):
        block, c = item(i)
        for n in range(0, cols, OUT_WIDTH):
            acc_ref[block, :, n:n + OUT_WIDTH] += jnp.dot(
                hidden_ref[f, i], wd_ref[f, c, :, n:n + OUT_WIDTH], preferred_element_type=jnp.float32)

    def pair_copy():
        return pltpu.make_async_remote_copy(
            src_ref=acc_ref.at[partner], dst_ref=pair_ref, send_sem=pair_send,
            recv_sem=pair_recv, device_id={"expert": partner}, device_id_type=MESH)

    def home_copy(k, t):
        return pltpu.make_async_remote_copy(
            src_ref=far_out_ref.at[k, t], dst_ref=far_in_ref.at[k, t], send_sem=home_send.at[k, t],
            recv_sem=home_recv.at[k, t], device_id={"expert": (same, other)[t][k]}, device_id_type=MESH)

    turn = RS_LAG * last
    total = items + turn + AG_LAG * last

    def step(s, carry):
        for f in order:
            i = s - RS_LAG * far_of(f)

            @pl.when((i >= 0) & (i < items))
            def _():
                reduce_item(f, i)

        for f in order:
            far = far_of(f)
            i = s - turn - AG_LAG * (last - far)

            @pl.when((i >= 0) & (i < items) & (far < last))
            def _():
                ag_copy(f, i).wait_recv()

                @pl.when(far > 0)
                def _():
                    ag_copy(f, i).start()

        prepare(s + 1)

        @pl.when(s == turn - 1)
        def _():
            scales()
            lax.fori_loop(0, half, wait_down, 0)

        for f in order:
            i = s - turn - AG_LAG * (last - far_of(f))

            @pl.when((i >= 0) & (i < items))
            def _():
                down(f, i)

        done = s - turn - AG_LAG * (last - nearest)
        for k in range(1, chips):
            for t in range(2):
                @pl.when(done == ends[2 * k + t])
                def _():
                    far_out_ref[k, t] = acc_ref[(same, other)[t][k]].astype(jnp.bfloat16)
                    home_copy(k, t).start()

        @pl.when(done == ends[-2])
        def _():
            pair_copy().start()

        return carry

    prepare(0)
    lax.fori_loop(0, total, step, 0)

    pair_copy().wait_recv()
    result = acc_ref[me] + pair_ref[...]
    for k in range(1, chips):
        for t in range(2):
            home_copy(k, t).wait_recv()
            result = result + far_in_ref[k, t].astype(jnp.float32)
    out_ref[...] = result.astype(jnp.bfloat16)

    for k in range(chips):
        tok_copy(k, me).wait_send()
        if k:
            pass_copy(k, same[k]).wait_send()
            for t in range(2):
                home_copy(k, t).wait_send()
    pair_copy().wait_send()
    for k in range(n_expert - 1):
        route_copy(k, me).wait_send()

    def drain(i, carry):
        for f in range(2):
            @pl.when(far_of(f) < last)
            def _():
                rs_copy(f, i).wait_send()

            @pl.when(far_of(f) > 0)
            def _():
                ag_copy(f, i).wait_send()

        return carry

    lax.fori_loop(0, items, drain, 0)


def every_expert(tokens, w_gate, w_up, w_down, expert_ids, route_weights):
    n_expert = lax.axis_size("expert")
    n_tensor = lax.axis_size("tensor")
    held, depth, ff = w_gate.shape
    tok_rows, cols = tokens.shape
    experts_all = n_expert * held
    half = held * (ff // CHUNK) // 2
    items = n_expert * half
    chips = n_expert // 2
    dma = pltpu.SemaphoreType.DMA
    vmem = pl.BlockSpec(memory_space=pltpu.VMEM)
    hbm = pl.BlockSpec(memory_space=pl.ANY)
    bf16 = jnp.bfloat16
    f32 = jnp.float32
    per_token = expert_ids.shape[1]
    return pl.pallas_call(
        functools.partial(layer_kernel, n_expert, n_tensor),
        out_shape=jax.ShapeDtypeStruct((tok_rows, cols), bf16),
        in_specs=[hbm] * 6,
        out_specs=vmem,
        scratch_shapes=[
            pltpu.VMEM((n_expert, tok_rows, cols), bf16),
            pltpu.VMEM((per_token, tok_rows), jnp.int32),
            pltpu.VMEM((per_token, tok_rows), f32),
            pltpu.VMEM((experts_all, tok_rows), f32),
            pltpu.VMEM((n_expert, experts_all, tok_rows), f32),
            pltpu.VMEM((held, n_expert, tok_rows, LANES), f32),
            pltpu.VMEM((2, half, depth, CHUNK), bf16),
            pltpu.VMEM((2, half, depth, CHUNK), bf16),
            pltpu.VMEM((2, half, CHUNK, cols), bf16),
            pltpu.VMEM((2, half, n_expert, tok_rows, 2 * CHUNK), f32),
            pltpu.VMEM((2, items, tok_rows, 2 * CHUNK), bf16),
            pltpu.VMEM((2, items, tok_rows, 2 * CHUNK), bf16),
            pltpu.VMEM((2, items, tok_rows, CHUNK), bf16),
            pltpu.VMEM((n_expert, tok_rows, cols), f32),
            pltpu.VMEM((tok_rows, cols), f32),
            pltpu.VMEM((chips, 2, tok_rows, cols), bf16),
            pltpu.VMEM((chips, 2, tok_rows, cols), bf16),
            dma((3,)),
            dma((2, 2, half)),
            dma((2, half)),
            dma((chips,)),
            dma((n_expert,)),
            dma((chips,)),
            dma((n_expert - 1,)),
            dma((n_expert,)),
            dma((2, items)),
            dma((2, items)),
            dma((2, items)),
            dma((2, items)),
            dma,
            dma,
            dma((chips, 2)),
            dma((chips, 2)),
        ],
        compiler_params=pltpu.CompilerParams(
            collective_id=0, has_side_effects=True, vmem_limit_bytes=56 * 1024 * 1024
        ),
    )(tokens, expert_ids.T, route_weights.T, w_gate, w_up, w_down)


def per_device(tokens, w_gate, w_up, w_down, expert_ids, route_weights):
    experts_all = w_gate.shape[0] * lax.axis_size("expert")
    if expert_ids.shape[1] == experts_all:
        return every_expert(tokens, w_gate, w_up, w_down, expert_ids, route_weights)
    return routed_by_slots(tokens, w_gate, w_up, w_down, expert_ids, route_weights)


def solution(mesh):
    in_specs = (
        P(("group", "expert"), "tensor"),
        P("expert", "tensor", None),
        P("expert", "tensor", None),
        P("expert", None, "tensor"),
        P(("group", "expert"), None),
        P(("group", "expert"), None),
    )
    out_specs = P(("group", "expert"), "tensor")
    return jax.shard_map(
        per_device, mesh=mesh, in_specs=in_specs, out_specs=out_specs, check_vma=False
    )
```

```python
import functools

import jax
import jax.numpy as jnp
from jax import lax
from jax.experimental import pallas as pl
from jax.experimental.pallas import tpu as pltpu
from jax.sharding import PartitionSpec as P


def slot_numbers(flat_ids, experts_all):
    labels = jnp.arange(experts_all, dtype=jnp.int32)
    onehot = (flat_ids[:, None] == labels[None, :]).astype(jnp.int32)
    before = jnp.cumsum(onehot, axis=0) - onehot
    return jnp.sum(before * onehot, axis=1)


def routed_by_slots(tokens, w_gate, w_up, w_down, expert_ids, route_weights):
    n_expert = lax.axis_size("expert")
    held_experts = w_gate.shape[0]
    experts_all = held_experts * n_expert
    tok_rows = tokens.shape[0]
    col_share = tokens.shape[1]
    per_token = expert_ids.shape[1]
    capacity = min(tok_rows, 2 * tok_rows * per_token // experts_all)
    flat_ids = expert_ids.reshape(tok_rows * per_token)
    position = flat_ids * capacity + slot_numbers(flat_ids, experts_all)
    owners = jnp.arange(tok_rows * per_token, dtype=jnp.int32) // per_token
    source = jnp.full((experts_all * capacity,), -1, jnp.int32).at[position].set(owners)
    filled = (source >= 0)[:, None]
    picked_rows = jnp.where(filled, tokens[jnp.maximum(source, 0)], jnp.zeros((), tokens.dtype))
    outgoing = picked_rows.reshape(n_expert, held_experts, capacity, col_share)
    received = lax.all_to_all(outgoing, "expert", split_axis=0, concat_axis=0, tiled=True)
    gate_part = jnp.einsum("sjnd,jdf->sjnf", received, w_gate, preferred_element_type=jnp.float32)
    up_part = jnp.einsum("sjnd,jdf->sjnf", received, w_up, preferred_element_type=jnp.float32)
    gate_share = lax.psum_scatter(gate_part, "tensor", scatter_dimension=3, tiled=True)
    up_share = lax.psum_scatter(up_part, "tensor", scatter_dimension=3, tiled=True)
    hidden_share = (jax.nn.silu(gate_share) * up_share).astype(jnp.bfloat16)
    hidden = lax.all_gather(hidden_share, "tensor", axis=3, tiled=True)
    result = jnp.einsum("sjnf,jfd->sjnd", hidden, w_down, preferred_element_type=jnp.float32)
    returned = result.astype(jnp.bfloat16)
    combined = lax.all_to_all(returned, "expert", split_axis=0, concat_axis=0, tiled=True).reshape(
        experts_all * capacity, col_share
    )
    picked = combined[position].reshape(tok_rows, per_token, col_share).astype(jnp.float32)
    mixed_out = jnp.sum(picked * route_weights[:, :, None], axis=1)
    return mixed_out.astype(jnp.bfloat16)


LANES = 128
CHUNK = 256
RS_HOP = 6
AG_HOP = 5
ALONE = 8
HEAD_LOADS = 2
SEND_LAG = 6
HEAD_OWN = 3
HEAD_PARTNER = 2
OUT_WIDTH = 512
MESH = pl.DeviceIdType.MESH


def layer_kernel(
    n_expert, n_tensor, tok_hbm, ids_hbm, weights_hbm, wg_hbm, wu_hbm, wd_hbm, out_ref,
    rows_ref, ids_ref, weights_ref, route_ref, routes_ref, scale_ref, wg_ref, wu_ref, wd_ref, part_ref, sent_ref,
    got_ref, hidden_ref, acc_ref, pair_ref, far_out_ref, far_in_ref,
    in_sem, w_sem, wd_sem, tok_send, tok_recv, pass_send, route_send, route_recv, rs_send, rs_recv, ag_send, ag_recv,
    pair_send, pair_recv, home_send, home_recv,
):
    held, depth, ff = wg_hbm.shape
    tok_rows, cols = tok_hbm.shape
    all_rows = n_expert * tok_rows
    per_expert = ff // CHUNK
    half = held * per_expert // 2
    items = n_expert * half
    me = lax.axis_index("expert")
    at = lax.axis_index("tensor")
    last = n_tensor - 1
    peers = [lax.rem(me + k, n_expert) for k in range(1, n_expert)]
    chips = n_expert // 2
    core = lax.rem(me, 2)
    chip = me // 2
    partner = 2 * chip + 1 - core
    same = [2 * lax.rem(chip + k, chips) + core for k in range(chips)]
    other = [2 * lax.rem(chip + k, chips) + 1 - core for k in range(chips)]

    segments = [(me, 0, HEAD_OWN), (partner, 0, HEAD_PARTNER)]
    for k in range(1, chips):
        segments += [(same[k], 0, half), (other[k], 0, half)]
    segments += [(partner, HEAD_PARTNER, half - HEAD_PARTNER), (me, HEAD_OWN, half - HEAD_OWN)]
    starts = [sum(count for _, _, count in segments[:n]) for n in range(len(segments))]
    ends = [start + segment[2] - 1 for start, segment in zip(starts, segments)]

    def item(i):
        block, chunk = me, i
        for start, (owner, first, _) in list(zip(starts, segments))[1:]:
            past = i >= start
            block = jnp.where(past, owner, block)
            chunk = jnp.where(past, i - start + first, chunk)
        return block, chunk

    def place(f, c):
        q = f * half + c
        return q // per_expert, pl.multiple_of(lax.rem(q, per_expert) * CHUNK, CHUNK)

    def w_copy(k, f, c):
        j, start = place(f, c)
        src = (wg_hbm, wu_hbm)[k].at[j, :, pl.ds(start, CHUNK)]
        return pltpu.make_async_copy(src, (wg_ref, wu_ref)[k].at[f, c], w_sem.at[k, f, c])

    def wd_copy(f, c):
        j, start = place(f, c)
        return pltpu.make_async_copy(wd_hbm.at[j, pl.ds(start, CHUNK), :], wd_ref.at[f, c], wd_sem.at[f, c])

    own_copies = [
        pltpu.make_async_copy(tok_hbm, rows_ref.at[me], in_sem.at[0]),
        pltpu.make_async_copy(ids_hbm, ids_ref, in_sem.at[1]),
        pltpu.make_async_copy(weights_hbm, weights_ref, in_sem.at[2]),
    ]
    for copy in own_copies:
        copy.start()
    for c in range(HEAD_LOADS):
        for f in range(2):
            for k in range(2):
                w_copy(k, f, c).start()

    barrier = pltpu.get_barrier_semaphore()
    for peer in peers:
        pl.semaphore_signal(barrier, inc=1, device_id={"expert": peer}, device_id_type=MESH)

    @pl.when(at > 0)
    def _():
        pl.semaphore_signal(barrier, inc=1, device_id={"tensor": at - 1}, device_id_type=MESH)

    @pl.when(at < last)
    def _():
        pl.semaphore_signal(barrier, inc=1, device_id={"tensor": at + 1}, device_id_type=MESH)

    for copy in own_copies:
        copy.wait()
    labels = lax.broadcasted_iota(jnp.int32, route_ref.shape, 0)
    routes = jnp.zeros(route_ref.shape, jnp.float32)
    for k in range(ids_ref.shape[0]):
        routes += jnp.where(ids_ref[k:k + 1, :] == labels, weights_ref[k:k + 1, :], 0.0)
    route_ref[...] = routes
    routes_ref[me] = routes

    greeted = (n_expert - 1) + (at > 0).astype(jnp.int32) + (at < last).astype(jnp.int32)
    pl.semaphore_wait(barrier, greeted)

    def tok_copy(k, slot):
        return pltpu.make_async_remote_copy(
            src_ref=rows_ref.at[slot], dst_ref=rows_ref.at[slot], send_sem=tok_send.at[k], recv_sem=tok_recv.at[slot],
            device_id={"expert": same[k] if k else partner}, device_id_type=MESH)

    def pass_copy(k, slot):
        return pltpu.make_async_remote_copy(
            src_ref=rows_ref.at[slot], dst_ref=rows_ref.at[slot], send_sem=pass_send.at[k],
            recv_sem=tok_recv.at[slot], device_id={"expert": partner}, device_id_type=MESH)

    def route_copy(k, slot):
        return pltpu.make_async_remote_copy(
            src_ref=route_ref, dst_ref=routes_ref.at[slot], send_sem=route_send.at[k], recv_sem=route_recv.at[slot],
            device_id={"expert": peers[k]}, device_id_type=MESH)

    for k in range(chips - 1, -1, -1):
        tok_copy(k, me).start()

    def load_rest(c, carry):
        for f in range(2):
            for k in range(2):
                w_copy(k, f, c).start()
        return carry

    def load_down(c, carry):
        for f in range(2):
            wd_copy(f, c).start()
        return carry

    def far_of(f):
        return jnp.where(f == 0, last - at, at)

    def onward(f):
        return jnp.where(f == 0, jnp.maximum(at - 1, 0), jnp.minimum(at + 1, last))

    def back(f):
        return jnp.where(f == 0, jnp.minimum(at + 1, last), jnp.maximum(at - 1, 0))

    near = jnp.where(at + at < n_tensor, 1, 0)
    order = (near, 1 - near)
    nearest = jnp.minimum(at, last - at)

    def rs_copy(f, i):
        return pltpu.make_async_remote_copy(
            src_ref=sent_ref.at[f, i], dst_ref=got_ref.at[f, i], send_sem=rs_send.at[f, i], recv_sem=rs_recv.at[f, i],
            device_id={"tensor": onward(f)}, device_id_type=MESH)

    def ag_copy(f, i):
        return pltpu.make_async_remote_copy(
            src_ref=hidden_ref.at[f, i], dst_ref=hidden_ref.at[f, i], send_sem=ag_send.at[f, i],
            recv_sem=ag_recv.at[f, i], device_id={"tensor": back(f)}, device_id_type=MESH)

    def wait_weights(c):
        for f in range(2):
            for k in range(2):
                w_copy(k, f, c).wait()

    def part_of_block(block, c):
        for f in range(2):
            for k, w_ref in enumerate((wg_ref, wu_ref)):
                part_ref[f, c, block, :, k * CHUNK:(k + 1) * CHUNK] = jnp.dot(
                    rows_ref[block], w_ref[f, c], preferred_element_type=jnp.float32)

    def part_of_all(c):
        for f in range(2):
            for k, w_ref in enumerate((wg_ref, wu_ref)):
                product = jnp.dot(
                    rows_ref[...].reshape(all_rows, depth), w_ref[f, c], preferred_element_type=jnp.float32)
                part_ref[f, c, :, :, k * CHUNK:(k + 1) * CHUNK] = product.reshape(n_expert, tok_rows, CHUNK)

    def prepare(i):
        @pl.when(i < HEAD_OWN)
        def _():
            wait_weights(i)

        @pl.when(i < HEAD_OWN + HEAD_PARTNER)
        def _():
            @pl.when(i == HEAD_OWN)
            def _():
                tok_copy(0, partner).wait_recv()

            block, c = item(i)
            part_of_block(block, c)

        @pl.when(i == HEAD_OWN + HEAD_PARTNER)
        def _():
            for k in range(1, chips):
                tok_copy(k, same[k]).wait_recv()
                pass_copy(k, same[k]).start()
            for k in range(1, chips):
                pass_copy(k, other[k]).wait_recv()

        @pl.when((i >= HEAD_OWN + HEAD_PARTNER) & (i < HEAD_OWN + HEAD_PARTNER + half))
        def _():
            c = i - (HEAD_OWN + HEAD_PARTNER)

            @pl.when(c >= HEAD_OWN)
            def _():
                wait_weights(c)

            part_of_all(c)

    def reduce_item(f, i):
        far = far_of(f)
        block, c = item(i)

        @pl.when(far == 0)
        def _():
            sent_ref[f, i] = part_ref[f, c, block].astype(jnp.bfloat16)

        @pl.when(far > 0)
        def _():
            rs_copy(f, i).wait_recv()

        @pl.when((far > 0) & (far < last))
        def _():
            sent_ref[f, i] = (part_ref[f, c, block] + got_ref[f, i].astype(jnp.float32)).astype(jnp.bfloat16)

        @pl.when(far < last)
        def _():
            rs_copy(f, i).start()

        @pl.when(far == last)
        def _():
            whole = part_ref[f, c, block] + got_ref[f, i].astype(jnp.float32)
            gate = whole[:, :CHUNK]
            up = whole[:, CHUNK:]
            j, _ = place(f, c)
            weight = jnp.concatenate([scale_ref[j, block]] * (CHUNK // LANES), axis=1)
            hidden_ref[f, i] = (jax.nn.silu(gate) * up * weight).astype(jnp.bfloat16)

    def scales():
        for k in range(n_expert - 1):
            route_copy(k, peers[k]).wait_recv()
        row = lax.broadcasted_iota(jnp.int32, (tok_rows, tok_rows), 0)
        column = lax.broadcasted_iota(jnp.int32, (tok_rows, tok_rows), 1)
        for j in range(held):
            for b in range(n_expert):
                mine = jnp.sum(
                    jnp.where(labels == me * held + j, routes_ref[b], 0.0), axis=0, keepdims=True)
                turned = jnp.sum(
                    jnp.where(row == column, jnp.broadcast_to(mine, (tok_rows, tok_rows)), 0.0), axis=1, keepdims=True)
                scale_ref[j, b] = jnp.broadcast_to(turned, (tok_rows, LANES))

    def wait_down(c, carry):
        for f in range(2):
            wd_copy(f, c).wait()
        return carry

    def down(f, i):
        block, c = item(i)
        for n in range(0, cols, OUT_WIDTH):
            acc_ref[block, :, n:n + OUT_WIDTH] += jnp.dot(
                hidden_ref[f, i], wd_ref[f, c, :, n:n + OUT_WIDTH], preferred_element_type=jnp.float32)

    def pair_copy():
        return pltpu.make_async_remote_copy(
            src_ref=acc_ref.at[partner], dst_ref=pair_ref, send_sem=pair_send,
            recv_sem=pair_recv, device_id={"expert": partner}, device_id_type=MESH)

    def home_copy(k, t):
        return pltpu.make_async_remote_copy(
            src_ref=far_out_ref.at[k, t], dst_ref=far_in_ref.at[k, t], send_sem=home_send.at[k, t],
            recv_sem=home_recv.at[k, t], device_id={"expert": (same, other)[t][k]}, device_id_type=MESH)

    turn = RS_HOP * last
    mixed = 2 * ALONE
    groups = (items - ALONE) // 2
    after = mixed + 5 * groups
    total = after + items - groups + AG_HOP * last

    def reduce_at(t):
        since = t - mixed
        place_in = lax.rem(jnp.maximum(since, 0), 5)
        early = (t >= 0) & (since < 0) & (lax.rem(jnp.maximum(t, 0), 2) == 0)
        later = (since >= 0) & (t < after) & ((place_in == 0) | (place_in == 2))
        i = jnp.where(since < 0, t // 2, ALONE + 2 * (since // 5) + place_in // 2)
        return jnp.where(early | later, i, -1)

    def gather_at(t):
        since = t - mixed
        beside = (since >= 0) & (t < after) & (lax.rem(jnp.maximum(since, 0), 5) == 4)
        alone = (t >= after) & (t < after + items - groups)
        i = jnp.where(t < after, since // 5, groups + t - after)
        return jnp.where(beside | alone, i, -1)

    def step(t, carry):
        for f in order:
            i = reduce_at(t - RS_HOP * far_of(f))

            @pl.when(i >= 0)
            def _():
                reduce_item(f, i)

        for f in order:
            far = far_of(f)
            i = gather_at(t - AG_HOP * (last - far))

            @pl.when(i >= 0)
            def _():
                @pl.when(far < last)
                def _():
                    ag_copy(f, i).wait_recv()

                @pl.when(far > 0)
                def _():
                    ag_copy(f, i).start()

        upcoming = reduce_at(t + 1)

        @pl.when(upcoming > 0)
        def _():
            prepare(upcoming)

        @pl.when(t == turn - 1)
        def _():
            scales()
            lax.fori_loop(0, half, wait_down, 0)

        for f in order:
            far = far_of(f)
            i = jnp.where(far == last, reduce_at(t - turn), gather_at(t - AG_HOP * (last - far)))

            @pl.when(i >= 0)
            def _():
                down(f, i)

        for f in order:
            far = far_of(f)
            i = gather_at(t - AG_HOP * (last - far))

            @pl.when((i >= 0) & (far < last))
            def _():
                rs_copy(f, i).wait_send()

            @pl.when((i >= SEND_LAG) & (far > 0))
            def _():
                ag_copy(f, i - SEND_LAG).wait_send()

        done = gather_at(t - AG_HOP * (last - nearest))

        @pl.when(t == 0)
        def _():
            for k in range(n_expert - 1):
                route_copy(k, me).start()
            lax.fori_loop(HEAD_LOADS, half, load_rest, 0)
            acc_ref[...] = jnp.zeros_like(acc_ref)

        @pl.when(t == 2 * HEAD_OWN)
        def _():
            lax.fori_loop(0, half, load_down, 0)

        for k in range(1, chips):
            for t_core in range(2):
                @pl.when(done == ends[2 * k + t_core])
                def _():
                    far_out_ref[k, t_core] = acc_ref[(same, other)[t_core][k]].astype(jnp.bfloat16)
                    home_copy(k, t_core).start()

        @pl.when(done == ends[-2])
        def _():
            pair_copy().start()

        return carry

    prepare(0)
    lax.fori_loop(0, total, step, 0)

    pair_copy().wait_recv()
    result = acc_ref[me] + pair_ref[...]
    for k in range(1, chips):
        for t in range(2):
            home_copy(k, t).wait_recv()
            result = result + far_in_ref[k, t].astype(jnp.float32)
    out_ref[...] = result.astype(jnp.bfloat16)

    for k in range(chips):
        tok_copy(k, me).wait_send()
        if k:
            pass_copy(k, same[k]).wait_send()
            for t in range(2):
                home_copy(k, t).wait_send()
    pair_copy().wait_send()
    for k in range(n_expert - 1):
        route_copy(k, me).wait_send()

    def drain(i, carry):
        for f in range(2):
            @pl.when(far_of(f) > 0)
            def _():
                ag_copy(f, i).wait_send()

        return carry

    lax.fori_loop(items - SEND_LAG, items, drain, 0)


def every_expert(tokens, w_gate, w_up, w_down, expert_ids, route_weights):
    n_expert = lax.axis_size("expert")
    n_tensor = lax.axis_size("tensor")
    held, depth, ff = w_gate.shape
    tok_rows, cols = tokens.shape
    experts_all = n_expert * held
    half = held * (ff // CHUNK) // 2
    items = n_expert * half
    chips = n_expert // 2
    dma = pltpu.SemaphoreType.DMA
    vmem = pl.BlockSpec(memory_space=pltpu.VMEM)
    hbm = pl.BlockSpec(memory_space=pl.ANY)
    bf16 = jnp.bfloat16
    f32 = jnp.float32
    per_token = expert_ids.shape[1]
    return pl.pallas_call(
        functools.partial(layer_kernel, n_expert, n_tensor),
        out_shape=jax.ShapeDtypeStruct((tok_rows, cols), bf16),
        in_specs=[hbm] * 6,
        out_specs=vmem,
        scratch_shapes=[
            pltpu.VMEM((n_expert, tok_rows, cols), bf16),
            pltpu.VMEM((per_token, tok_rows), jnp.int32),
            pltpu.VMEM((per_token, tok_rows), f32),
            pltpu.VMEM((experts_all, tok_rows), f32),
            pltpu.VMEM((n_expert, experts_all, tok_rows), f32),
            pltpu.VMEM((held, n_expert, tok_rows, LANES), f32),
            pltpu.VMEM((2, half, depth, CHUNK), bf16),
            pltpu.VMEM((2, half, depth, CHUNK), bf16),
            pltpu.VMEM((2, half, CHUNK, cols), bf16),
            pltpu.VMEM((2, half, n_expert, tok_rows, 2 * CHUNK), f32),
            pltpu.VMEM((2, items, tok_rows, 2 * CHUNK), bf16),
            pltpu.VMEM((2, items, tok_rows, 2 * CHUNK), bf16),
            pltpu.VMEM((2, items, tok_rows, CHUNK), bf16),
            pltpu.VMEM((n_expert, tok_rows, cols), f32),
            pltpu.VMEM((tok_rows, cols), f32),
            pltpu.VMEM((chips, 2, tok_rows, cols), bf16),
            pltpu.VMEM((chips, 2, tok_rows, cols), bf16),
            dma((3,)),
            dma((2, 2, half)),
            dma((2, half)),
            dma((chips,)),
            dma((n_expert,)),
            dma((chips,)),
            dma((n_expert - 1,)),
            dma((n_expert,)),
            dma((2, items)),
            dma((2, items)),
            dma((2, items)),
            dma((2, items)),
            dma,
            dma,
            dma((chips, 2)),
            dma((chips, 2)),
        ],
        compiler_params=pltpu.CompilerParams(
            collective_id=0, has_side_effects=True, vmem_limit_bytes=56 * 1024 * 1024
        ),
    )(tokens, expert_ids.T, route_weights.T, w_gate, w_up, w_down)


def per_device(tokens, w_gate, w_up, w_down, expert_ids, route_weights):
    experts_all = w_gate.shape[0] * lax.axis_size("expert")
    if expert_ids.shape[1] == experts_all:
        return every_expert(tokens, w_gate, w_up, w_down, expert_ids, route_weights)
    return routed_by_slots(tokens, w_gate, w_up, w_down, expert_ids, route_weights)


def solution(mesh):
    in_specs = (
        P(("group", "expert"), "tensor"),
        P("expert", "tensor", None),
        P("expert", "tensor", None),
        P("expert", None, "tensor"),
        P(("group", "expert"), None),
        P(("group", "expert"), None),
    )
    out_specs = P(("group", "expert"), "tensor")
    return jax.shard_map(
        per_device, mesh=mesh, in_specs=in_specs, out_specs=out_specs, check_vma=False
    )
```

```python
import functools

import jax
import jax.numpy as jnp
from jax import lax
from jax.experimental import pallas as pl
from jax.experimental.pallas import tpu as pltpu
from jax.sharding import PartitionSpec as P


def slot_numbers(flat_ids, experts_all):
    labels = jnp.arange(experts_all, dtype=jnp.int32)
    onehot = (flat_ids[:, None] == labels[None, :]).astype(jnp.int32)
    before = jnp.cumsum(onehot, axis=0) - onehot
    return jnp.sum(before * onehot, axis=1)


def routed_by_slots(tokens, w_gate, w_up, w_down, expert_ids, route_weights):
    n_expert = lax.axis_size("expert")
    held_experts = w_gate.shape[0]
    experts_all = held_experts * n_expert
    tok_rows = tokens.shape[0]
    col_share = tokens.shape[1]
    per_token = expert_ids.shape[1]
    capacity = min(tok_rows, 2 * tok_rows * per_token // experts_all)
    flat_ids = expert_ids.reshape(tok_rows * per_token)
    position = flat_ids * capacity + slot_numbers(flat_ids, experts_all)
    owners = jnp.arange(tok_rows * per_token, dtype=jnp.int32) // per_token
    source = jnp.full((experts_all * capacity,), -1, jnp.int32).at[position].set(owners)
    filled = (source >= 0)[:, None]
    picked_rows = jnp.where(filled, tokens[jnp.maximum(source, 0)], jnp.zeros((), tokens.dtype))
    outgoing = picked_rows.reshape(n_expert, held_experts, capacity, col_share)
    received = lax.all_to_all(outgoing, "expert", split_axis=0, concat_axis=0, tiled=True)
    gate_part = jnp.einsum("sjnd,jdf->sjnf", received, w_gate, preferred_element_type=jnp.float32)
    up_part = jnp.einsum("sjnd,jdf->sjnf", received, w_up, preferred_element_type=jnp.float32)
    gate_share = lax.psum_scatter(gate_part, "tensor", scatter_dimension=3, tiled=True)
    up_share = lax.psum_scatter(up_part, "tensor", scatter_dimension=3, tiled=True)
    hidden_share = (jax.nn.silu(gate_share) * up_share).astype(jnp.bfloat16)
    hidden = lax.all_gather(hidden_share, "tensor", axis=3, tiled=True)
    result = jnp.einsum("sjnf,jfd->sjnd", hidden, w_down, preferred_element_type=jnp.float32)
    returned = result.astype(jnp.bfloat16)
    combined = lax.all_to_all(returned, "expert", split_axis=0, concat_axis=0, tiled=True).reshape(
        experts_all * capacity, col_share
    )
    picked = combined[position].reshape(tok_rows, per_token, col_share).astype(jnp.float32)
    mixed_out = jnp.sum(picked * route_weights[:, :, None], axis=1)
    return mixed_out.astype(jnp.bfloat16)


LANES = 128
CHUNK = 256
RS_HOP = 6
AG_HOP = 6
ALONE = 8
RS_SLOTS = 12
AG_SLOTS = 20
HEAD_OWN = 3
HEAD_PARTNER = 2
OUT_WIDTH = 512
MESH = pl.DeviceIdType.MESH


def layer_kernel(
    n_expert, n_tensor, tok_hbm, ids_hbm, weights_hbm, wg_hbm, wu_hbm, wd_hbm, out_ref,
    rows_ref, ids_ref, weights_ref, route_ref, routes_ref, scale_ref, w_ref, wd_ref, part_ref, sent_ref,
    got_ref, hidden_ref, acc_ref, pair_ref, far_out_ref, far_in_ref,
    in_sem, w_sem, wd_sem, tok_send, tok_recv, pass_send, route_send, route_recv, rs_send, rs_recv, ag_send, ag_recv,
    pair_send, pair_recv, home_send, home_recv,
):
    held, depth, ff = wg_hbm.shape
    tok_rows, cols = tok_hbm.shape
    all_rows = n_expert * tok_rows
    per_expert = ff // CHUNK
    half = held * per_expert // 2
    items = n_expert * half
    me = lax.axis_index("expert")
    at = lax.axis_index("tensor")
    last = n_tensor - 1
    peers = [lax.rem(me + k, n_expert) for k in range(1, n_expert)]
    chips = n_expert // 2
    core = lax.rem(me, 2)
    chip = me // 2
    partner = 2 * chip + 1 - core
    same = [2 * lax.rem(chip + k, chips) + core for k in range(chips)]
    other = [2 * lax.rem(chip + k, chips) + 1 - core for k in range(chips)]

    segments = [(me, 0, HEAD_OWN), (partner, 0, HEAD_PARTNER)]
    for k in range(1, chips):
        segments += [(same[k], 0, half), (other[k], 0, half)]
    segments += [(partner, HEAD_PARTNER, half - HEAD_PARTNER), (me, HEAD_OWN, half - HEAD_OWN)]
    starts = [sum(count for _, _, count in segments[:n]) for n in range(len(segments))]
    ends = [start + segment[2] - 1 for start, segment in zip(starts, segments)]

    def item(i):
        block, chunk = me, i
        for start, (owner, first, _) in list(zip(starts, segments))[1:]:
            past = i >= start
            block = jnp.where(past, owner, block)
            chunk = jnp.where(past, i - start + first, chunk)
        return block, chunk

    def place(f, c):
        q = f * half + c
        return q // per_expert, pl.multiple_of(lax.rem(q, per_expert) * CHUNK, CHUNK)

    def w_copy(k, f, c):
        j, start = place(f, c)
        src = (wg_hbm, wu_hbm)[k].at[j, :, pl.ds(start, CHUNK)]
        return pltpu.make_async_copy(src, w_ref.at[c, f, k], w_sem.at[c])

    def load_chunk(c):
        for f in range(2):
            for k in range(2):
                w_copy(k, f, c).start()

    load_down = pltpu.make_async_copy(wd_hbm, wd_ref, wd_sem)

    own_copies = [
        pltpu.make_async_copy(tok_hbm, rows_ref.at[me], in_sem.at[0]),
        pltpu.make_async_copy(ids_hbm, ids_ref, in_sem.at[1]),
        pltpu.make_async_copy(weights_hbm, weights_ref, in_sem.at[2]),
    ]
    for copy in own_copies:
        copy.start()
    load_chunk(0)

    barrier = pltpu.get_barrier_semaphore()
    for peer in peers:
        pl.semaphore_signal(barrier, inc=1, device_id={"expert": peer}, device_id_type=MESH)

    @pl.when(at > 0)
    def _():
        pl.semaphore_signal(barrier, inc=1, device_id={"tensor": at - 1}, device_id_type=MESH)

    @pl.when(at < last)
    def _():
        pl.semaphore_signal(barrier, inc=1, device_id={"tensor": at + 1}, device_id_type=MESH)

    own_copies[0].wait()
    greeted = (n_expert - 1) + (at > 0).astype(jnp.int32) + (at < last).astype(jnp.int32)
    pl.semaphore_wait(barrier, greeted)

    def tok_copy(k, slot):
        return pltpu.make_async_remote_copy(
            src_ref=rows_ref.at[slot], dst_ref=rows_ref.at[slot], send_sem=tok_send.at[k], recv_sem=tok_recv.at[slot],
            device_id={"expert": same[k] if k else partner}, device_id_type=MESH)

    def pass_copy(k, slot):
        return pltpu.make_async_remote_copy(
            src_ref=rows_ref.at[slot], dst_ref=rows_ref.at[slot], send_sem=pass_send.at[k],
            recv_sem=tok_recv.at[slot], device_id={"expert": partner}, device_id_type=MESH)

    def route_copy(k, slot):
        return pltpu.make_async_remote_copy(
            src_ref=route_ref, dst_ref=routes_ref.at[slot], send_sem=route_send.at[k], recv_sem=route_recv.at[slot],
            device_id={"expert": peers[k]}, device_id_type=MESH)

    for k in range(chips - 1, -1, -1):
        tok_copy(k, me).start()
    load_chunk(1)

    def load_rest(c, carry):
        load_chunk(c)
        return carry

    def send_routes():
        for copy in own_copies[1:]:
            copy.wait()
        routes = jnp.zeros(route_ref.shape, jnp.float32)
        for k in range(ids_ref.shape[0]):
            routes += jnp.where(ids_ref[k:k + 1, :] == labels, weights_ref[k:k + 1, :], 0.0)
        route_ref[...] = routes
        routes_ref[me] = routes
        for k in range(n_expert - 1):
            route_copy(k, me).start()

    labels = lax.broadcasted_iota(jnp.int32, route_ref.shape, 0)

    def far_of(f):
        return jnp.where(f == 0, last - at, at)

    def onward(f):
        return jnp.where(f == 0, jnp.maximum(at - 1, 0), jnp.minimum(at + 1, last))

    def back(f):
        return jnp.where(f == 0, jnp.minimum(at + 1, last), jnp.maximum(at - 1, 0))

    near = jnp.where(at + at < n_tensor, 1, 0)
    order = (near, 1 - near)
    nearest = jnp.minimum(at, last - at)

    def rs_copy(f, i):
        return pltpu.make_async_remote_copy(
            src_ref=sent_ref.at[f, i], dst_ref=got_ref.at[f, i], send_sem=rs_send.at[f],
            recv_sem=rs_recv.at[f, lax.rem(i, RS_SLOTS)], device_id={"tensor": onward(f)}, device_id_type=MESH)

    def ag_copy(f, i):
        return pltpu.make_async_remote_copy(
            src_ref=hidden_ref.at[f, i], dst_ref=hidden_ref.at[f, i], send_sem=ag_send.at[f],
            recv_sem=ag_recv.at[f, lax.rem(i, AG_SLOTS)], device_id={"tensor": back(f)}, device_id_type=MESH)

    def all_sent(ref, sem):
        return pltpu.make_async_remote_copy(
            src_ref=ref, dst_ref=ref, send_sem=sem, recv_sem=rs_recv.at[0, 0],
            device_id={"tensor": onward(0)}, device_id_type=MESH)

    def wait_weights(c):
        pltpu.make_async_copy(w_ref.at[c], w_ref.at[c], w_sem.at[c]).wait()

    def part_of_block(block, c):
        for f in range(2):
            for k in range(2):
                part_ref[f, c, block, :, k * CHUNK:(k + 1) * CHUNK] = jnp.dot(
                    rows_ref[block], w_ref[c, f, k], preferred_element_type=jnp.float32)

    def part_of_all(c):
        for f in range(2):
            for k in range(2):
                product = jnp.dot(
                    rows_ref[...].reshape(all_rows, depth), w_ref[c, f, k], preferred_element_type=jnp.float32)
                part_ref[f, c, :, :, k * CHUNK:(k + 1) * CHUNK] = product.reshape(n_expert, tok_rows, CHUNK)

    def prepare(i):
        @pl.when(i < HEAD_OWN)
        def _():
            wait_weights(i)

        @pl.when(i < HEAD_OWN + HEAD_PARTNER)
        def _():
            @pl.when(i == HEAD_OWN)
            def _():
                tok_copy(0, partner).wait_recv()

            block, c = item(i)
            part_of_block(block, c)

        @pl.when(i == HEAD_OWN + HEAD_PARTNER)
        def _():
            for k in range(1, chips):
                tok_copy(k, same[k]).wait_recv()
                pass_copy(k, same[k]).start()
            for k in range(1, chips):
                pass_copy(k, other[k]).wait_recv()

        @pl.when((i >= HEAD_OWN + HEAD_PARTNER) & (i < HEAD_OWN + HEAD_PARTNER + half))
        def _():
            c = i - (HEAD_OWN + HEAD_PARTNER)

            @pl.when(c >= HEAD_OWN)
            def _():
                wait_weights(c)

            part_of_all(c)

    def reduce_item(f, i):
        far = far_of(f)
        block, c = item(i)

        @pl.when(far == 0)
        def _():
            sent_ref[f, i] = part_ref[f, c, block].astype(jnp.bfloat16)

        @pl.when(far > 0)
        def _():
            rs_copy(f, i).wait_recv()

        @pl.when((far > 0) & (far < last))
        def _():
            sent_ref[f, i] = (part_ref[f, c, block] + got_ref[f, i].astype(jnp.float32)).astype(jnp.bfloat16)

        @pl.when(far < last)
        def _():
            rs_copy(f, i).start()

        @pl.when(far == last)
        def _():
            whole = part_ref[f, c, block] + got_ref[f, i].astype(jnp.float32)
            gate = whole[:, :CHUNK]
            up = whole[:, CHUNK:]
            j, _ = place(f, c)
            weight = jnp.concatenate([scale_ref[j, block]] * (CHUNK // LANES), axis=1)
            hidden_ref[f, i] = (jax.nn.silu(gate) * up * weight).astype(jnp.bfloat16)

    def scales():
        for k in range(n_expert - 1):
            route_copy(k, peers[k]).wait_recv()
        row = lax.broadcasted_iota(jnp.int32, (tok_rows, tok_rows), 0)
        column = lax.broadcasted_iota(jnp.int32, (tok_rows, tok_rows), 1)
        for j in range(held):
            for b in range(n_expert):
                mine = jnp.sum(
                    jnp.where(labels == me * held + j, routes_ref[b], 0.0), axis=0, keepdims=True)
                turned = jnp.sum(
                    jnp.where(row == column, jnp.broadcast_to(mine, (tok_rows, tok_rows)), 0.0), axis=1, keepdims=True)
                scale_ref[j, b] = jnp.broadcast_to(turned, (tok_rows, LANES))

    def down(f, i):
        block, c = item(i)
        j, start = place(f, c)
        for n in range(0, cols, OUT_WIDTH):
            acc_ref[block, :, n:n + OUT_WIDTH] += jnp.dot(
                hidden_ref[f, i], wd_ref[j, pl.ds(start, CHUNK), n:n + OUT_WIDTH], preferred_element_type=jnp.float32)

    def pair_copy():
        return pltpu.make_async_remote_copy(
            src_ref=acc_ref.at[partner], dst_ref=pair_ref, send_sem=pair_send,
            recv_sem=pair_recv, device_id={"expert": partner}, device_id_type=MESH)

    def home_copy(k, t):
        return pltpu.make_async_remote_copy(
            src_ref=far_out_ref.at[k, t], dst_ref=far_in_ref.at[k, t], send_sem=home_send.at[k, t],
            recv_sem=home_recv.at[k, t], device_id={"expert": (same, other)[t][k]}, device_id_type=MESH)

    turn = RS_HOP * last
    mixed = 2 * ALONE
    groups = (items - ALONE) // 2
    after = mixed + 5 * groups
    total = after + items - groups + AG_HOP * last

    def reduce_at(t):
        since = t - mixed
        place_in = lax.rem(jnp.maximum(since, 0), 5)
        early = (t >= 0) & (since < 0) & (lax.rem(jnp.maximum(t, 0), 2) == 0)
        later = (since >= 0) & (t < after) & ((place_in == 0) | (place_in == 2))
        i = jnp.where(since < 0, t // 2, ALONE + 2 * (since // 5) + place_in // 2)
        return jnp.where(early | later, i, -1)

    def gather_at(t):
        since = t - mixed
        beside = (since >= 0) & (t < after) & (lax.rem(jnp.maximum(since, 0), 5) == 4)
        alone = (t >= after) & (t < after + items - groups)
        i = jnp.where(t < after, since // 5, groups + t - after)
        return jnp.where(beside | alone, i, -1)

    def step(t, carry):
        for f in order:
            i = reduce_at(t - RS_HOP * far_of(f))

            @pl.when(i >= 0)
            def _():
                reduce_item(f, i)

        for f in order:
            far = far_of(f)
            i = gather_at(t - AG_HOP * (last - far))

            @pl.when(i >= 0)
            def _():
                @pl.when(far < last)
                def _():
                    ag_copy(f, i).wait_recv()

                @pl.when(far > 0)
                def _():
                    ag_copy(f, i).start()

        upcoming = reduce_at(t + 1)

        @pl.when(upcoming > 0)
        def _():
            prepare(upcoming)

        @pl.when(t == turn - 1)
        def _():
            scales()
            load_down.wait()

        for f in order:
            far = far_of(f)
            i = jnp.where(far == last, reduce_at(t - turn), gather_at(t - AG_HOP * (last - far)))

            @pl.when(i >= 0)
            def _():
                down(f, i)

        done = gather_at(t - AG_HOP * (last - nearest))

        @pl.when(t == 0)
        def _():
            lax.fori_loop(2, half, load_rest, 0)
            send_routes()
            acc_ref[...] = jnp.zeros_like(acc_ref)

        @pl.when(t == 2 * HEAD_OWN)
        def _():
            load_down.start()

        for k in range(1, chips):
            for t_core in range(2):
                @pl.when(done == ends[2 * k + t_core])
                def _():
                    far_out_ref[k, t_core] = acc_ref[(same, other)[t_core][k]].astype(jnp.bfloat16)
                    home_copy(k, t_core).start()

        @pl.when(done == ends[-2])
        def _():
            pair_copy().start()

        return carry

    prepare(0)
    lax.fori_loop(0, total, step, 0)

    pair_copy().wait_recv()
    result = acc_ref[me] + pair_ref[...]
    for k in range(1, chips):
        for t in range(2):
            home_copy(k, t).wait_recv()
            result = result + far_in_ref[k, t].astype(jnp.float32)
    out_ref[...] = result.astype(jnp.bfloat16)

    for k in range(chips):
        tok_copy(k, me).wait_send()
        if k:
            pass_copy(k, same[k]).wait_send()
            for t in range(2):
                home_copy(k, t).wait_send()
    pair_copy().wait_send()
    for k in range(n_expert - 1):
        route_copy(k, me).wait_send()

    for f in range(2):
        @pl.when(far_of(f) < last)
        def _():
            all_sent(sent_ref.at[f], rs_send.at[f]).wait_send()

        @pl.when(far_of(f) > 0)
        def _():
            all_sent(hidden_ref.at[f], ag_send.at[f]).wait_send()


def every_expert(tokens, w_gate, w_up, w_down, expert_ids, route_weights):
    n_expert = lax.axis_size("expert")
    n_tensor = lax.axis_size("tensor")
    held, depth, ff = w_gate.shape
    tok_rows, cols = tokens.shape
    experts_all = n_expert * held
    half = held * (ff // CHUNK) // 2
    items = n_expert * half
    chips = n_expert // 2
    dma = pltpu.SemaphoreType.DMA
    vmem = pl.BlockSpec(memory_space=pltpu.VMEM)
    hbm = pl.BlockSpec(memory_space=pl.ANY)
    bf16 = jnp.bfloat16
    f32 = jnp.float32
    per_token = expert_ids.shape[1]
    return pl.pallas_call(
        functools.partial(layer_kernel, n_expert, n_tensor),
        out_shape=jax.ShapeDtypeStruct((tok_rows, cols), bf16),
        in_specs=[hbm] * 6,
        out_specs=vmem,
        scratch_shapes=[
            pltpu.VMEM((n_expert, tok_rows, cols), bf16),
            pltpu.VMEM((per_token, tok_rows), jnp.int32),
            pltpu.VMEM((per_token, tok_rows), f32),
            pltpu.VMEM((experts_all, tok_rows), f32),
            pltpu.VMEM((n_expert, experts_all, tok_rows), f32),
            pltpu.VMEM((held, n_expert, tok_rows, LANES), f32),
            pltpu.VMEM((half, 2, 2, depth, CHUNK), bf16),
            pltpu.VMEM(w_down.shape, bf16),
            pltpu.VMEM((2, half, n_expert, tok_rows, 2 * CHUNK), f32),
            pltpu.VMEM((2, items, tok_rows, 2 * CHUNK), bf16),
            pltpu.VMEM((2, items, tok_rows, 2 * CHUNK), bf16),
            pltpu.VMEM((2, items, tok_rows, CHUNK), bf16),
            pltpu.VMEM((n_expert, tok_rows, cols), f32),
            pltpu.VMEM((tok_rows, cols), f32),
            pltpu.VMEM((chips, 2, tok_rows, cols), bf16),
            pltpu.VMEM((chips, 2, tok_rows, cols), bf16),
            dma((3,)),
            dma((half,)),
            dma,
            dma((chips,)),
            dma((n_expert,)),
            dma((chips,)),
            dma((n_expert - 1,)),
            dma((n_expert,)),
            dma((2,)),
            dma((2, RS_SLOTS)),
            dma((2,)),
            dma((2, AG_SLOTS)),
            dma,
            dma,
            dma((chips, 2)),
            dma((chips, 2)),
        ],
        compiler_params=pltpu.CompilerParams(
            collective_id=0, has_side_effects=True, vmem_limit_bytes=56 * 1024 * 1024
        ),
    )(tokens, expert_ids.T, route_weights.T, w_gate, w_up, w_down)


def per_device(tokens, w_gate, w_up, w_down, expert_ids, route_weights):
    experts_all = w_gate.shape[0] * lax.axis_size("expert")
    if expert_ids.shape[1] == experts_all:
        return every_expert(tokens, w_gate, w_up, w_down, expert_ids, route_weights)
    return routed_by_slots(tokens, w_gate, w_up, w_down, expert_ids, route_weights)


def solution(mesh):
    in_specs = (
        P(("group", "expert"), "tensor"),
        P("expert", "tensor", None),
        P("expert", "tensor", None),
        P("expert", None, "tensor"),
        P(("group", "expert"), None),
        P(("group", "expert"), None),
    )
    out_specs = P(("group", "expert"), "tensor")
    return jax.shard_map(
        per_device, mesh=mesh, in_specs=in_specs, out_specs=out_specs, check_vma=False
    )
```
